32 devices in a mesh: dp: 8 (over z, y), tensor: 4 (over x, core).
Axes of the slice: x: 2, y: 2, z: 4, core: 2. Of those that a mesh axis runs over, the one named last changes fastest.
Arguments:
- out_grad: bfloat16 [2048, 1024], P('dp'), may hold values from -0.29882812 to 0.29882812
- hidden: bfloat16 [2048, 28672], P('dp', 'tensor'), may hold values from -60 to 60
- momentum: float32 [1024, 28672], P('dp', 'tensor'), may hold values from -48 to 48
- second: float32 [1024], P('dp'), may hold values from 0.01 to 0.2
Outputs:
- update: bfloat16 [1024, 28672], P('dp', 'tensor')
- momentum_out: float32 [1024, 28672], P('dp', 'tensor')
- second_out: float32 [1024], P('dp')
The draws below stay inside these ranges and needn't reach their ends.
All inputs are finite; a program needn't handle non-finite values.
Results may differ from the reference program's by a relative error of at most 0.035.
Values may be sent and summed in bfloat16 or wider, within the bound.
A program may use at most 128 MiB of HBM per device.

```python
import math
import jax
import jax.numpy as jnp
from jax import lax

FF = 28672
ROWS_DEV = 128
ITERS = 3
ROWS = 1024
TOKENS = 2048
N_DP = 8


def draw_hidden(key, part):
    first_key = jax.random.fold_in(jax.random.fold_in(key, 17), 0)
    column_ramp = jnp.exp(jnp.log(3.0) * jnp.arange(FF, dtype=jnp.float32) / FF)
    base_values = jnp.clip(jax.random.normal(first_key, (TOKENS, FF), jnp.float32), -6.0, 6.0)
    return (base_values * column_ramp[None, :]).astype(jnp.bfloat16)


def with_spikes(drawn, stream_key, source, target, blocks, factor):
    owner, partner = [(jnp.arange(drawn.shape[position]) // (drawn.shape[position] // blocks)).reshape([-1 if axis == position else 1 for axis in range(drawn.ndim)]) for position in (source, target)]
    chosen = jax.random.permutation(stream_key, blocks)[partner]
    strong = (owner == chosen) | (owner == (partner + blocks // 2) % blocks)
    return jnp.where(strong, factor * drawn, drawn)


def shard_levels(own_key, dims, cuts, low, top_value):
    factor_of, own = 1.0, jax.random.fold_in(own_key, 6)
    for dim, shards_of in cuts:
        heights = jnp.exp(jax.random.uniform(jax.random.fold_in(own, dim), (shards_of,), jnp.float32, low / len(cuts), top_value / len(cuts)))
        factor_of = factor_of * jnp.repeat(heights, dims[dim] // shards_of).reshape([-1 if axis == dim else 1 for axis in range(len(dims))])
    return factor_of


def normal_values(rng, dims, width, limit, cuts=(), held_as=jnp.bfloat16):
    array = jax.random.normal(rng, dims, jnp.float32) * width
    if len(cuts) > 0:
        array = shard_levels(rng, dims, cuts, -0.22, 0.18) * array
    return jnp.clip(array, min=-limit, max=limit).astype(held_as)


def heavy_noise(stream_key, dims, width, bound, shards, heavy, kind=jnp.bfloat16):
    entries = width * jax.random.normal(stream_key, dims, jnp.float32)
    if shards:
        entries = entries * shard_levels(stream_key, dims, shards, -0.22, 0.18)
    return jnp.clip(with_spikes(entries, jax.random.fold_in(stream_key, 3), *heavy), -bound, bound).astype(kind)


def setup_inputs(seed: int = 0) -> dict:
    splits = jax.random.split(jax.random.key(seed), 5)
    out_grad = heavy_noise(splits[0], (TOKENS, ROWS), 0.05, 0.29882812, ((0, 8),), (0, 1, 8, 2.0))
    hidden = draw_hidden(jax.random.fold_in(splits[4], 71), 0)
    momentum = normal_values(splits[2], (ROWS, FF), 8.0, 48.0, ((0, 8), (1, 4)), jnp.float32)
    second = jnp.clip(jnp.exp(math.log(0.2) - 2.9957323 * jax.random.uniform(splits[3], (ROWS,), jnp.float32) ** shard_levels(splits[3], (ROWS,), ((0, 8),), -0.2, 0.2)), 0.01, 0.2)
    return dict(out_grad=out_grad, hidden=hidden, momentum=momentum, second=second)


quintic_a = 3.4445
quintic_b = -4.775
quintic_c = 2.0315
beta_one = 0.95
beta_two = 0.95

def orthogonal_panel(panel):
    norm_sum = jnp.sqrt(jnp.sum(panel * panel))
    current = (panel / (norm_sum + 1e-07)).astype(jnp.bfloat16)
    for iteration in range(ITERS):
        gram = jnp.dot(current, current.T, preferred_element_type=jnp.float32).astype(jnp.bfloat16)
        square = jnp.dot(gram, gram, preferred_element_type=jnp.float32)
        poly = (quintic_b * gram.astype(jnp.float32) + quintic_c * square).astype(jnp.bfloat16)
        current = (quintic_a * current.astype(jnp.float32) + jnp.dot(poly, current, preferred_element_type=jnp.float32)).astype(jnp.bfloat16)
    return current

def reference(out_grad, hidden, momentum, second):
    tok_block = out_grad.shape[0] // N_DP
    grad_blocks = out_grad.reshape(N_DP, tok_block, out_grad.shape[1])
    hidden_blocks = hidden.reshape(N_DP, tok_block, hidden.shape[1])

    def add_block(running, pair):
        grad_block, hidden_block = pair
        partial_term = lax.dot_general(grad_block, hidden_block, (((0,), (0,)), ((), ())), preferred_element_type=jnp.float32)
        rounded = lax.optimization_barrier(partial_term.astype(jnp.bfloat16))
        return (running + rounded.astype(jnp.float32), None)
    start_sum = jnp.zeros((out_grad.shape[1], hidden.shape[1]), jnp.float32)
    grad, unused = lax.scan(add_block, start_sum, (grad_blocks, hidden_blocks))
    momentum_out = beta_one * momentum + grad
    nesterov = grad + beta_one * momentum_out
    panels = nesterov.reshape(N_DP, ROWS_DEV, FF)
    orthogonal = lax.map(orthogonal_panel, panels).reshape(ROWS_DEV * N_DP, FF)
    ortho_wide = orthogonal.astype(jnp.float32)
    energy = lax.optimization_barrier(jnp.sum(ortho_wide * ortho_wide, axis=1))
    second_out = beta_two * second + (1.0 - beta_two) * energy
    update = (ortho_wide * jnp.sqrt(FF / second_out)[:, None]).astype(jnp.bfloat16)
    return (update, momentum_out, second_out)
```

```python
import functools

import jax
import jax.numpy as jnp
from jax import lax
from jax.experimental import pallas as pl
from jax.experimental.pallas import tpu as pltpu
from jax.sharding import PartitionSpec as P

ITERS = 3
quintic_a = 3.4445
quintic_b = -4.775
quintic_c = 2.0315
beta_one = 0.95
beta_two = 0.95

MESH = pl.DeviceIdType.MESH
F32 = jnp.float32
BF16 = jnp.bfloat16


def line_split(n_dp):
    ny = 1
    while ny * ny * 4 <= n_dp and n_dp % (ny * 2) == 0:
        ny *= 2
    return n_dp // ny, ny


def exact_dot(a, b):
    return jnp.dot(a, b, preferred_element_type=F32, precision=lax.Precision.HIGHEST)


def kernel(
    nz, ny, nt, n_chunks, ff,
    og_hbm, h_hbm, mom_hbm, sec_ref,
    upd_hbm, momout_hbm, secout_ref,
    h, ograw, og_t, rr, rl, sr, sl, mom, x, gram, norm, g_all,
    h_sem, og_sem, y_send, og_send, rr_sem, rl_sem, sr_sem, sl_sem, mom_sem, momout_sem, upd_sem,
    g_send, g_recv,
):
    tokens = h_hbm.shape[0]
    rows, width = x.shape[1], x.shape[2]
    d = lax.axis_index("dp")
    t = lax.axis_index("tensor")
    z, y = d // ny, lax.rem(d, ny)

    def at_y(k):
        return (z * ny + lax.rem(y + k, ny), t)

    def at_z(step):
        return (d + step * ny, t)

    def at_t(k):
        return (d, lax.rem(t + k, nt))

    barrier = pltpu.get_barrier_semaphore()
    for k in range(1, ny):
        pl.semaphore_signal(barrier, inc=1, device_id=at_y(k), device_id_type=MESH)
    for k in range(1, nt):
        pl.semaphore_signal(barrier, inc=1, device_id=at_t(k), device_id_type=MESH)

    @pl.when(z > 0)
    def _():
        pl.semaphore_signal(barrier, inc=1, device_id=at_z(-1), device_id_type=MESH)

    @pl.when(z < nz - 1)
    def _():
        pl.semaphore_signal(barrier, inc=1, device_id=at_z(1), device_id_type=MESH)

    mine = pl.ds(pl.multiple_of(y * tokens, tokens), tokens)
    for j in range(nz):
        cols = pl.ds(pl.multiple_of((j * ny + y) * rows, rows), rows)
        pltpu.make_async_copy(og_hbm.at[:, cols], ograw.at[y, j], og_sem.at[y]).start()

    def columns(c):
        return pl.ds(pl.multiple_of(c * width, width), width)

    def own_load(c, carry):
        pltpu.make_async_copy(h_hbm.at[:, columns(c)], h.at[c, mine], h_sem.at[y, c]).start()
        return carry

    lax.fori_loop(0, n_chunks, own_load, 0)

    ends = jnp.minimum(z, 1) + jnp.minimum(nz - 1 - z, 1)
    pl.semaphore_wait(barrier, (ny - 1) + (nt - 1) + ends)

    for k in range(1, ny):
        peer = lax.rem(y + k, ny)
        for j in range(nz):
            cols = pl.ds(pl.multiple_of((j * ny + peer) * rows, rows), rows)
            pltpu.make_async_remote_copy(
                og_hbm.at[:, cols], ograw.at[y, j], og_send.at[k - 1], og_sem.at[y],
                device_id=at_y(k), device_id_type=MESH,
            ).start()

    def y_sends(c, carry):
        for k in range(1, ny):
            pltpu.make_async_remote_copy(
                h_hbm.at[:, columns(c)], h.at[c, mine], y_send.at[k - 1], h_sem.at[y, c],
                device_id=at_y(k), device_id_type=MESH,
            ).start()
        return carry

    lax.fori_loop(0, n_chunks, y_sends, 0)

    def mom_load(c, carry):
        pltpu.make_async_copy(mom_hbm.at[:, columns(c)], mom.at[c], mom_sem).start()
        return carry

    lax.fori_loop(0, n_chunks, mom_load, 0)
    gram[...] = jnp.zeros_like(gram)
    norm[...] = jnp.zeros_like(norm)
    for k in range(ny):
        pltpu.make_async_copy(ograw.at[k], ograw.at[k], og_sem.at[k]).wait()
    for k in range(ny):
        for j in range(nz):
            og_t[j, :, k * tokens : (k + 1) * tokens] = ograw[k, j].T
    pltpu.make_async_copy(mom, mom, mom_sem).wait()

    def partial(j, c):
        return jnp.dot(og_t[j], h[c], preferred_element_type=F32)

    def send_on(j, c, slot, first, recv, recv_sem, send, send_sem, step):
        own = partial(j, c)

        @pl.when(first)
        def _():
            send[slot, c] = own.astype(BF16)

        @pl.when(jnp.logical_not(first))
        def _():
            pltpu.make_async_copy(recv.at[slot, c], recv.at[slot, c], recv_sem.at[slot, c]).wait()
            send[slot, c] = (own + recv[slot, c].astype(F32)).astype(BF16)

        pltpu.make_async_remote_copy(
            send.at[slot, c], recv.at[slot, c], send_sem.at[slot], recv_sem.at[slot, c],
            device_id=at_z(step), device_id_type=MESH,
        ).start()

    reach = jnp.maximum(z, nz - 1 - z)

    def step(s, carry):
        @pl.when(s < n_chunks)
        def _():
            for k in range(ny):
                block = h.at[s, pl.ds(k * tokens, tokens)]
                pltpu.make_async_copy(block, block, h_sem.at[k, s]).wait()

        right = s - z

        @pl.when(jnp.logical_and(right >= 0, right < n_chunks))
        def _():
            for j in range(nz - 1, 0, -1):
                @pl.when(z < j)
                def _():
                    send_on(j, right, j - 1, z == 0, rr, rr_sem, sr, sr_sem, 1)

        left = s - (nz - 1 - z)

        @pl.when(jnp.logical_and(left >= 0, left < n_chunks))
        def _():
            for j in range(nz - 1):
                @pl.when(z > j)
                def _():
                    send_on(j, left, j, z == nz - 1, rl, rl_sem, sl, sl_sem, -1)

        c = s - reach

        @pl.when(jnp.logical_and(c >= 0, c < n_chunks))
        def _():
            x_grad = norm.at[1]
            x_grad[...] = partial(z, c)

            @pl.when(z > 0)
            def _():
                pltpu.make_async_copy(rr.at[z - 1, c], rr.at[z - 1, c], rr_sem.at[z - 1, c]).wait()
                x_grad[...] += rr[z - 1, c].astype(F32)

            @pl.when(z < nz - 1)
            def _():
                pltpu.make_async_copy(rl.at[z, c], rl.at[z, c], rl_sem.at[z, c]).wait()
                x_grad[...] += rl[z, c].astype(F32)

            grad = x_grad[...]
            momentum_out = beta_one * mom[c] + grad
            nesterov = grad + beta_one * momentum_out
            mom[c] = momentum_out
            pltpu.make_async_copy(mom.at[c], momout_hbm.at[:, columns(c)], momout_sem).start()
            panel = nesterov.astype(BF16)
            x[c] = panel
            norm[0] += nesterov * nesterov
            gram[...] += lax.dot_general(
                panel, panel, (((1,), (1,)), ((), ())), preferred_element_type=F32
            )

        return carry

    lax.fori_loop(0, n_chunks + nz - 1, step, 0)

    g_all[t, :rows] = gram[...]
    total = jnp.sum(jnp.sum(norm[0], axis=0, keepdims=True), axis=1, keepdims=True)
    g_all[t, rows:] = jnp.broadcast_to(total, (8, rows))
    for k in range(1, nt):
        pltpu.make_async_remote_copy(
            g_all.at[t], g_all.at[t], g_send.at[k - 1], g_recv.at[t],
            device_id=at_t(k), device_id_type=MESH,
        ).start()
    for k in range(nt):
        @pl.when(k != t)
        def _():
            pltpu.make_async_copy(g_all.at[k], g_all.at[k], g_recv.at[k]).wait()
    summed = g_all[0]
    for k in range(1, nt):
        summed = summed + g_all[k]
    inverse = 1.0 / (jnp.sqrt(summed[rows : rows + 1]) + 1e-07)
    current = summed[:rows] * inverse * inverse
    eye = (
        lax.broadcasted_iota(jnp.int32, (rows, rows), 0)
        == lax.broadcasted_iota(jnp.int32, (rows, rows), 1)
    ).astype(F32)
    map_all = None
    for _ in range(ITERS):
        square = exact_dot(current, current)
        map_one = quintic_a * eye + quintic_b * current + quintic_c * square
        map_all = map_one if map_all is None else exact_dot(map_one, map_all)
        current = exact_dot(map_one, exact_dot(current, map_one))
    energy = jnp.sum(current * eye, axis=0, keepdims=True)
    second_out = beta_two * sec_ref[...] + (1.0 - beta_two) * energy
    secout_ref[...] = second_out
    scale = jnp.sqrt(ff / second_out) * inverse
    final = jnp.sum(eye * scale, axis=1, keepdims=True) * map_all
    high = final.astype(BF16)
    low = (final - high.astype(F32)).astype(BF16)

    def finish(c, carry):
        panel = x[c]
        out = jnp.dot(high, panel, preferred_element_type=F32)
        out += jnp.dot(low, panel, preferred_element_type=F32)
        x[c] = out.astype(BF16)
        pltpu.make_async_copy(x.at[c], upd_hbm.at[:, columns(c)], upd_sem).start()
        return carry

    lax.fori_loop(0, n_chunks, finish, 0)

    pltpu.make_async_copy(mom, mom, momout_sem).wait()
    for k in range(1, ny):
        pltpu.make_async_copy(ograw.at[0], ograw.at[0], og_send.at[k - 1]).wait()
        blocks = h.at[:, pl.ds(0, tokens)]
        pltpu.make_async_copy(blocks, blocks, y_send.at[k - 1]).wait()
    for j in range(1, nz):
        @pl.when(z < j)
        def _():
            pltpu.make_async_copy(sr.at[j - 1], sr.at[j - 1], sr_sem.at[j - 1]).wait()
    for j in range(nz - 1):
        @pl.when(z > j)
        def _():
            pltpu.make_async_copy(sl.at[j], sl.at[j], sl_sem.at[j]).wait()
    for k in range(1, nt):
        pltpu.make_async_copy(g_all.at[0], g_all.at[0], g_send.at[k - 1]).wait()
    pltpu.make_async_copy(x, x, upd_sem).wait()


def body(nz, ny, nt, out_grad, hidden, momentum, second):
    tokens, cols = hidden.shape
    rows = momentum.shape[0]
    width = 256 if cols % 256 == 0 else 128
    n_chunks = cols // width
    dma = pltpu.SemaphoreType.DMA
    anywhere = pl.BlockSpec(memory_space=pl.ANY)
    vmem = pl.BlockSpec(memory_space=pltpu.VMEM)
    hops = (nz - 1, n_chunks)
    update, momentum_out, second_out = pl.pallas_call(
        functools.partial(kernel, nz, ny, nt, n_chunks, float(cols * nt)),
        out_shape=(
            jax.ShapeDtypeStruct((rows, cols), BF16),
            jax.ShapeDtypeStruct((rows, cols), F32),
            jax.ShapeDtypeStruct((1, rows), F32),
        ),
        in_specs=[anywhere, anywhere, anywhere, vmem],
        out_specs=(anywhere, anywhere, vmem),
        scratch_shapes=[
            pltpu.VMEM((n_chunks, ny * tokens, width), BF16),
            pltpu.VMEM((ny, nz, tokens, rows), BF16),
            pltpu.VMEM((nz, rows, ny * tokens), BF16),
            pltpu.VMEM(hops + (rows, width), BF16),
            pltpu.VMEM(hops + (rows, width), BF16),
            pltpu.VMEM(hops + (rows, width), BF16),
            pltpu.VMEM(hops + (rows, width), BF16),
            pltpu.VMEM((n_chunks, rows, width), F32),
            pltpu.VMEM((n_chunks, rows, width), BF16),
            pltpu.VMEM((rows, rows), F32),
            pltpu.VMEM((2, rows, width), F32),
            pltpu.VMEM((nt, rows + 8, rows), F32),
            dma((ny, n_chunks)),
            dma((ny,)),
            dma((max(ny - 1, 1),)),
            dma((max(ny - 1, 1),)),
            dma(hops),
            dma(hops),
            dma((nz - 1,)),
            dma((nz - 1,)),
            dma,
            dma,
            dma,
            dma((max(nt - 1, 1),)),
            dma((nt,)),
        ],
        compiler_params=pltpu.CompilerParams(
            collective_id=0, has_side_effects=True, vmem_limit_bytes=60 * 1024 * 1024
        ),
        name="normuon",
    )(out_grad, hidden, momentum, second.reshape(1, rows))
    return update, momentum_out, second_out.reshape(rows)


def solution(mesh):
    nz, ny = line_split(mesh.shape["dp"])
    placed = (P("dp", None), P("dp", "tensor"), P("dp", "tensor"), P("dp"))
    return jax.shard_map(
        functools.partial(body, nz, ny, mesh.shape["tensor"]),
        mesh=mesh,
        in_specs=placed,
        out_specs=(P("dp", "tensor"), P("dp", "tensor"), P("dp")),
        check_vma=False,
    )
```

```python
import functools

import jax
import jax.numpy as jnp
from jax import lax
from jax.experimental import pallas as pl
from jax.experimental.pallas import tpu as pltpu
from jax.sharding import PartitionSpec as P

ITERS = 3
quintic_a = 3.4445
quintic_b = -4.775
quintic_c = 2.0315
beta_one = 0.95
beta_two = 0.95

MESH = pl.DeviceIdType.MESH
F32 = jnp.float32
BF16 = jnp.bfloat16


def line_split(n_dp):
    ny = 1
    while ny * ny * 4 <= n_dp and n_dp % (ny * 2) == 0:
        ny *= 2
    return n_dp // ny, ny


def exact_dot(a, b):
    return jnp.dot(a, b, preferred_element_type=F32, precision=lax.Precision.HIGHEST)


def kernel(
    nz, ny, nt, n_chunks, ff,
    og_hbm, h_hbm, mom_hbm, sec_ref,
    x, mom, final_ref, secout_ref,
    h, ograw, og_t, rr, rl, sr, sl, gram, norm, g_all,
    h_sem, og_sem, y_send, og_send, rr_sem, rl_sem, sr_sem, sl_sem, mom_sem,
    g_send, g_recv,
):
    tokens = h_hbm.shape[0]
    rows, width = x.shape[1], x.shape[2]
    d = lax.axis_index("dp")
    t = lax.axis_index("tensor")
    z, y = d // ny, lax.rem(d, ny)

    def at_y(k):
        return (z * ny + lax.rem(y + k, ny), t)

    def at_z(step):
        return (d + step * ny, t)

    def at_t(k):
        return (d, lax.rem(t + k, nt))

    barrier = pltpu.get_barrier_semaphore()
    for k in range(1, ny):
        pl.semaphore_signal(barrier, inc=1, device_id=at_y(k), device_id_type=MESH)
    for k in range(1, nt):
        pl.semaphore_signal(barrier, inc=1, device_id=at_t(k), device_id_type=MESH)

    @pl.when(z > 0)
    def _():
        pl.semaphore_signal(barrier, inc=1, device_id=at_z(-1), device_id_type=MESH)

    @pl.when(z < nz - 1)
    def _():
        pl.semaphore_signal(barrier, inc=1, device_id=at_z(1), device_id_type=MESH)

    mine = pl.ds(pl.multiple_of(y * tokens, tokens), tokens)

    def columns(c):
        return pl.ds(pl.multiple_of(c * width, width), width)

    ends = jnp.minimum(z, 1) + jnp.minimum(nz - 1 - z, 1)
    pl.semaphore_wait(barrier, (ny - 1) + (nt - 1) + ends)

    def far_first(i):
        return jnp.where(z * 2 < nz, nz - 1 - i, i)

    def og_sends(i):
        j = far_first(i)
        for k in range(1, ny):
            peer = lax.rem(y + k, ny)
            cols = pl.ds(pl.multiple_of((j * ny + peer) * rows, rows), rows)
            pltpu.make_async_remote_copy(
                og_hbm.at[:, cols], ograw.at[y, j], og_send.at[k - 1], og_sem.at[y, j],
                device_id=at_y(k), device_id_type=MESH,
            ).start()

    def y_sends(c, carry):
        for k in range(1, ny):
            pltpu.make_async_remote_copy(
                h_hbm.at[:, columns(c)], h.at[c, mine], y_send.at[k - 1], h_sem.at[y, c],
                device_id=at_y(k), device_id_type=MESH,
            ).start()
        return carry

    og_sends(0)
    y_sends(0, 0)
    for i in range(1, nz):
        og_sends(i)
    lax.fori_loop(1, n_chunks, y_sends, 0)

    for j in range(nz):
        cols = pl.ds(pl.multiple_of((j * ny + y) * rows, rows), rows)
        pltpu.make_async_copy(og_hbm.at[:, cols], ograw.at[y, j], og_sem.at[y, j]).start()

    def own_load(c, carry):
        pltpu.make_async_copy(h_hbm.at[:, columns(c)], h.at[c, mine], h_sem.at[y, c]).start()
        return carry

    lax.fori_loop(0, n_chunks, own_load, 0)

    def mom_load(c, carry):
        pltpu.make_async_copy(mom_hbm.at[:, columns(c)], mom.at[c], mom_sem).start()
        return carry

    lax.fori_loop(0, n_chunks, mom_load, 0)
    gram[...] = jnp.zeros_like(gram)
    norm[...] = jnp.zeros_like(norm)
    pltpu.make_async_copy(mom, mom, mom_sem).wait()

    def prepare(j):
        for k in range(ny):
            pltpu.make_async_copy(ograw.at[k, j], ograw.at[k, j], og_sem.at[k, j]).wait()
            og_t[j, :, k * tokens : (k + 1) * tokens] = ograw[k, j].T

    def partial(j, c):
        return jnp.dot(og_t[j], h[c], preferred_element_type=F32)

    def send_on(j, c, slot, first, recv, recv_sem, send, send_sem, step):
        own = partial(j, c)

        @pl.when(first)
        def _():
            send[slot, c] = own.astype(BF16)

        @pl.when(jnp.logical_not(first))
        def _():
            pltpu.make_async_copy(recv.at[slot, c], recv.at[slot, c], recv_sem.at[slot, c]).wait()
            send[slot, c] = (own + recv[slot, c].astype(F32)).astype(BF16)

        pltpu.make_async_remote_copy(
            send.at[slot, c], recv.at[slot, c], send_sem.at[slot], recv_sem.at[slot, c],
            device_id=at_z(step), device_id_type=MESH,
        ).start()

    reach = jnp.maximum(z, nz - 1 - z)

    def step(s, carry):
        @pl.when(s < n_chunks)
        def _():
            for k in range(ny):
                block = h.at[s, pl.ds(k * tokens, tokens)]
                pltpu.make_async_copy(block, block, h_sem.at[k, s]).wait()

        right = s - z

        @pl.when(jnp.logical_and(right >= 0, right < n_chunks))
        def _():
            for j in range(nz - 1, 0, -1):
                @pl.when(z < j)
                def _():
                    @pl.when(s == 0)
                    def _():
                        prepare(j)

                    send_on(j, right, j - 1, z == 0, rr, rr_sem, sr, sr_sem, 1)

        left = s - (nz - 1 - z)

        @pl.when(jnp.logical_and(left >= 0, left < n_chunks))
        def _():
            for j in range(nz - 1):
                @pl.when(z > j)
                def _():
                    @pl.when(s == 0)
                    def _():
                        prepare(j)

                    send_on(j, left, j, z == nz - 1, rl, rl_sem, sl, sl_sem, -1)

        for j in range(nz):
            inner = jnp.logical_and(z > 0, z < nz - 1)

            @pl.when(jnp.logical_and(s == 0, jnp.logical_or(inner, z == j)))
            def _():
                prepare(j)

        c = s - reach

        @pl.when(jnp.logical_and(c >= 0, c < n_chunks))
        def _():
            x_grad = norm.at[1]
            x_grad[...] = partial(z, c)

            @pl.when(z > 0)
            def _():
                pltpu.make_async_copy(rr.at[z - 1, c], rr.at[z - 1, c], rr_sem.at[z - 1, c]).wait()
                x_grad[...] += rr[z - 1, c].astype(F32)

            @pl.when(z < nz - 1)
            def _():
                pltpu.make_async_copy(rl.at[z, c], rl.at[z, c], rl_sem.at[z, c]).wait()
                x_grad[...] += rl[z, c].astype(F32)

            grad = x_grad[...]
            momentum_out = beta_one * mom[c] + grad
            nesterov = grad + beta_one * momentum_out
            mom[c] = momentum_out
            panel = nesterov.astype(BF16)
            x[c] = panel
            norm[0] += nesterov * nesterov
            gram[...] += lax.dot_general(
                panel, panel, (((1,), (1,)), ((), ())), preferred_element_type=F32
            )

        return carry

    lax.fori_loop(0, n_chunks + nz - 1, step, 0)

    g_all[t, :rows] = gram[...]
    total = jnp.sum(jnp.sum(norm[0], axis=0, keepdims=True), axis=1, keepdims=True)
    g_all[t, rows:] = jnp.broadcast_to(total, (8, rows))
    for k in range(1, nt):
        pltpu.make_async_remote_copy(
            g_all.at[t], g_all.at[t], g_send.at[k - 1], g_recv.at[t],
            device_id=at_t(k), device_id_type=MESH,
        ).start()
    for k in range(nt):
        @pl.when(k != t)
        def _():
            pltpu.make_async_copy(g_all.at[k], g_all.at[k], g_recv.at[k]).wait()
    summed = g_all[0]
    for k in range(1, nt):
        summed = summed + g_all[k]
    inverse = 1.0 / (jnp.sqrt(summed[rows : rows + 1]) + 1e-07)
    current = summed[:rows] * inverse * inverse
    eye = (
        lax.broadcasted_iota(jnp.int32, (rows, rows), 0)
        == lax.broadcasted_iota(jnp.int32, (rows, rows), 1)
    ).astype(F32)
    map_all = None
    for iteration in range(ITERS):
        square = exact_dot(current, current)
        map_one = quintic_a * eye + quintic_b * current + quintic_c * square
        map_all = map_one if map_all is None else exact_dot(map_one, map_all)
        mapped = exact_dot(map_one, current)
        if iteration < ITERS - 1:
            current = exact_dot(mapped, map_one)
    energy = jnp.sum(mapped * map_one, axis=0, keepdims=True)
    second_out = beta_two * sec_ref[...] + (1.0 - beta_two) * energy
    secout_ref[...] = second_out
    scale = jnp.sqrt(ff / second_out) * inverse
    final = jnp.sum(eye * scale, axis=1, keepdims=True) * map_all
    final_ref[...] = final

    for k in range(1, ny):
        pltpu.make_async_copy(ograw.at[0], ograw.at[0], og_send.at[k - 1]).wait()
        blocks = h.at[:, pl.ds(0, tokens)]
        pltpu.make_async_copy(blocks, blocks, y_send.at[k - 1]).wait()
    for j in range(1, nz):
        @pl.when(z < j)
        def _():
            pltpu.make_async_copy(sr.at[j - 1], sr.at[j - 1], sr_sem.at[j - 1]).wait()
    for j in range(nz - 1):
        @pl.when(z > j)
        def _():
            pltpu.make_async_copy(sl.at[j], sl.at[j], sl_sem.at[j]).wait()
    for k in range(1, nt):
        pltpu.make_async_copy(g_all.at[0], g_all.at[0], g_send.at[k - 1]).wait()


def write_kernel(n_chunks, x, mom, final_ref, sec_ref, upd_hbm, momout_hbm, secout_ref, out, mom_sem, upd_sem):
    width = x.shape[2]

    def columns(c):
        return pl.ds(pl.multiple_of(c * width, width), width)

    high = final_ref[...].astype(BF16)
    low = (final_ref[...] - high.astype(F32)).astype(BF16)
    secout_ref[...] = sec_ref[...]

    def finish(c, carry):
        pltpu.make_async_copy(mom.at[c], momout_hbm.at[:, columns(c)], mom_sem).start()
        panel = x[c]
        result = jnp.dot(high, panel, preferred_element_type=F32)
        result += jnp.dot(low, panel, preferred_element_type=F32)
        out[c] = result.astype(BF16)
        pltpu.make_async_copy(out.at[c], upd_hbm.at[:, columns(c)], upd_sem).start()
        return carry

    lax.fori_loop(0, n_chunks, finish, 0)
    pltpu.make_async_copy(mom, mom, mom_sem).wait()
    pltpu.make_async_copy(out, out, upd_sem).wait()


def body(nz, ny, nt, out_grad, hidden, momentum, second):
    tokens, cols = hidden.shape
    rows = momentum.shape[0]
    width = 256 if cols % 256 == 0 else 128
    n_chunks = cols // width
    dma = pltpu.SemaphoreType.DMA
    anywhere = pl.BlockSpec(memory_space=pltpu.HBM)
    vmem = pl.BlockSpec(memory_space=pltpu.VMEM)
    hops = (nz - 1, n_chunks)
    panel, mom, final, second_out = pl.pallas_call(
        functools.partial(kernel, nz, ny, nt, n_chunks, float(cols * nt)),
        out_shape=(
            jax.ShapeDtypeStruct((n_chunks, rows, width), BF16),
            jax.ShapeDtypeStruct((n_chunks, rows, width), F32),
            jax.ShapeDtypeStruct((rows, rows), F32),
            jax.ShapeDtypeStruct((1, rows), F32),
        ),
        in_specs=[anywhere, anywhere, anywhere, vmem],
        out_specs=(vmem, vmem, vmem, vmem),
        scratch_shapes=[
            pltpu.VMEM((n_chunks, ny * tokens, width), BF16),
            pltpu.VMEM((ny, nz, tokens, rows), BF16),
            pltpu.VMEM((nz, rows, ny * tokens), BF16),
            pltpu.VMEM(hops + (rows, width), BF16),
            pltpu.VMEM(hops + (rows, width), BF16),
            pltpu.VMEM(hops + (rows, width), BF16),
            pltpu.VMEM(hops + (rows, width), BF16),
            pltpu.VMEM((rows, rows), F32),
            pltpu.VMEM((2, rows, width), F32),
            pltpu.VMEM((nt, rows + 8, rows), F32),
            dma((ny, n_chunks)),
            dma((ny, nz)),
            dma((max(ny - 1, 1),)),
            dma((max(ny - 1, 1),)),
            dma(hops),
            dma(hops),
            dma((nz - 1,)),
            dma((nz - 1,)),
            dma,
            dma((max(nt - 1, 1),)),
            dma((nt,)),
        ],
        compiler_params=pltpu.CompilerParams(
            collective_id=0, has_side_effects=True, vmem_limit_bytes=47 * 1024 * 1024
        ),
        name="normuon",
    )(out_grad, hidden, momentum, second.reshape(1, rows))
    update, momentum_out, second_out = pl.pallas_call(
        functools.partial(write_kernel, n_chunks),
        out_shape=(
            jax.ShapeDtypeStruct((rows, cols), BF16),
            jax.ShapeDtypeStruct((rows, cols), F32),
            jax.ShapeDtypeStruct((1, rows), F32),
        ),
        in_specs=[vmem] * 4,
        out_specs=(anywhere, anywhere, vmem),
        scratch_shapes=[pltpu.VMEM((n_chunks, rows, width), BF16), dma, dma],
        compiler_params=pltpu.CompilerParams(vmem_limit_bytes=16 * 1024 * 1024),
        name="write_results",
    )(panel, mom, final, second_out)
    return update, momentum_out, second_out.reshape(rows)


def solution(mesh):
    nz, ny = line_split(mesh.shape["dp"])
    placed = (P("dp", None), P("dp", "tensor"), P("dp", "tensor"), P("dp"))
    return jax.shard_map(
        functools.partial(body, nz, ny, mesh.shape["tensor"]),
        mesh=mesh,
        in_specs=placed,
        out_specs=(P("dp", "tensor"), P("dp", "tensor"), P("dp")),
        check_vma=False,
    )
```
